32 devices in a mesh: rep: 2 (over x), dp: 16 (over y, z, core).
Axes of the slice: x: 2, y: 2, z: 4, core: 2. Of those that a mesh axis runs over, the one named last changes fastest.
Arguments:
- x: bfloat16 [32, 1024, 512], P(('rep', 'dp')), parts along dimension 0
- dy: bfloat16 [32, 1024, 512], P(('rep', 'dp')), parts along dimension 0
- w_gate: bfloat16 [2, 512, 8192], P(None, 'dp')
- w_up: bfloat16 [2, 512, 8192], P(None, 'dp')
- w_down: bfloat16 [2, 8192, 512], P(None, 'dp')
- m_w_gate: float32 [2, 512, 8192], P(None, 'dp')
- m_w_up: float32 [2, 512, 8192], P(None, 'dp')
- m_w_down: float32 [2, 8192, 512], P(None, 'dp')
- v_w_gate: float32 [2, 512, 8192], P(None, 'dp')
- v_w_up: float32 [2, 512, 8192], P(None, 'dp')
- v_w_down: float32 [2, 8192, 512], P(None, 'dp')
Outputs:
- output 1: bfloat16 [4, 512, 8192], P('rep', 'dp'), parts along dimension 0
- output 2: bfloat16 [4, 512, 8192], P('rep', 'dp'), parts along dimension 0
- output 3: bfloat16 [4, 8192, 512], P('rep', 'dp'), parts along dimension 0
- output 4: float32 [4, 512, 8192], P('rep', 'dp'), parts along dimension 0
- output 5: float32 [4, 512, 8192], P('rep', 'dp'), parts along dimension 0
- output 6: float32 [4, 8192, 512], P('rep', 'dp'), parts along dimension 0
- output 7: float32 [4, 512, 8192], P('rep', 'dp'), parts along dimension 0
- output 8: float32 [4, 512, 8192], P('rep', 'dp'), parts along dimension 0
- output 9: float32 [4, 8192, 512], P('rep', 'dp'), parts along dimension 0
There are 2 independent parts. The reference program is written for one: setup_inputs(seed, part) draws one part's arguments, and reference() takes and returns one part's arrays. A program takes and returns all parts, laid end to end along the dimension named above; an argument that names none is the same for every part.
All inputs are finite; a program needn't handle non-finite values.
Results may differ from the reference program's by a relative error of at most 0.022.
Values are sent between devices in bfloat16 or wider.
A program may use at most 2 GiB of HBM per device.

```python
import jax
import jax.numpy as jnp
from jax import lax

SEQUENCES = 16
TOKENS = 1024
D = 512
FF = 8192
LAYERS = 2
NAMES = ("w_gate", "w_up", "w_down")
SHAPES = {"w_gate": (LAYERS, D, FF), "w_up": (LAYERS, D, FF), "w_down": (LAYERS, FF, D)}


def bump(key, n, height):
    away = (jnp.arange(n, dtype=jnp.int32) - jax.random.randint(key, (), 0, n, jnp.int32)) % n
    return jnp.where(away < n // 8, height, 1.0)


def together(key, own, strength):
    shared = jax.random.normal(key, own.shape[1:], jnp.float32)
    return (own + strength * shared) * lax.rsqrt(1 + strength * strength)


def setup_inputs(seed: int = 0, part: int = 0) -> dict:
    kx, kdy, ka, kb, kz, kf, kh, kl, *keys = jax.random.split(jax.random.key(seed), 8 + 3 * len(NAMES))
    kx, kdy, ka, kb = (jax.random.fold_in(k, part) for k in (kx, kdy, ka, kb))
    kw, km, kv = (keys[i::3] for i in range(3))
    shape = (SEQUENCES, TOKENS, D)
    much_x, much_dy = jax.random.uniform(kz, (2,), jnp.float32, 0.0, 1.0)
    loud = 2.0 ** jax.random.uniform(jax.random.fold_in(kz, 1), (), jnp.float32, -1.0, 2.0)
    layers = 2.0 ** jax.random.uniform(kl, (LAYERS, 1, 1), jnp.float32, -1.0, 1.0)
    x = together(ka, jax.random.normal(kx, shape, jnp.float32), much_x) * bump(kf, D, 4.0)
    dy = together(kb, jax.random.normal(kdy, shape, jnp.float32), much_dy)
    drawn = {"x": x.astype(jnp.bfloat16), "dy": (loud * dy * (SEQUENCES * TOKENS) ** -0.5).astype(jnp.bfloat16)}
    for key, name in zip(kw, NAMES, strict=True):
        w = jax.random.normal(key, SHAPES[name], jnp.float32) * SHAPES[name][1] ** -0.5
        drawn[name] = (w * {"w_gate": 1.0, "w_up": bump(kh, FF, 4.0), "w_down": layers}[name]).astype(jnp.bfloat16)
    for key, name in zip(km, NAMES, strict=True):
        drawn[f"m_{name}"] = 0.1 * jax.random.normal(key, SHAPES[name], jnp.float32)
    for key, name in zip(kv, NAMES, strict=True):
        drawn[f"v_{name}"] = jax.random.uniform(key, SHAPES[name], jnp.float32, 0.005, 0.015)
    return drawn


def matmul(a, w):
    return jnp.dot(a, w, preferred_element_type=jnp.float32).astype(jnp.bfloat16)


def normed(h):
    wide = h.astype(jnp.float32)
    scale = lax.rsqrt(jnp.mean(wide**2, -1, keepdims=True) + 1e-6)
    return (wide * scale).astype(jnp.bfloat16)


def layer(h, w):
    a = normed(h)
    gate = jnp.dot(a, w["w_gate"], preferred_element_type=jnp.float32)
    up = jnp.dot(a, w["w_up"], preferred_element_type=jnp.float32)
    return h + matmul((jax.nn.silu(gate) * up).astype(jnp.bfloat16), w["w_down"])


def adamw(w, m, v, g):
    m = 0.9 * m + 0.1 * g
    v = 0.95 * v + 0.05 * g * g
    step = m * lax.rsqrt(v + 1e-8) + 0.1 * w
    return (w - 0.02 * step).astype(jnp.bfloat16), m, v


def clipped(gradients, sum_of_squares, count):
    factor = jnp.minimum(1.0, 0.5 * lax.rsqrt(sum_of_squares / count + 1e-30))
    return [g * factor for g in gradients]


def stack(weights, h):
    return lax.scan(lambda h, w: (layer(h, w), None), h, weights)[0]


def reference(x, dy, w_gate, w_up, w_down, m_w_gate, m_w_up, m_w_down, v_w_gate, v_w_up, v_w_down):
    weights = dict(zip(NAMES, (w_gate, w_up, w_down), strict=True))

    def take(so_far, sequence):
        h, by_y = sequence
        _, back = jax.vjp(lambda w: stack(w, h), weights)
        return jax.tree.map(lambda total, term: total + term.astype(jnp.float32), so_far, back(by_y)[0]), None

    none_yet = {name: jnp.zeros(w.shape, jnp.float32) for name, w in weights.items()}
    by_weights, _ = lax.scan(take, none_yet, (x, dy))
    gradients = [by_weights[name].astype(jnp.bfloat16).astype(jnp.float32) for name in NAMES]
    gradients = clipped(gradients, sum(jnp.sum(g * g) for g in gradients), sum(g.size for g in gradients))
    new = [
        adamw(w.astype(jnp.float32), m, v, g)
        for w, m, v, g in zip((w_gate, w_up, w_down), (m_w_gate, m_w_up, m_w_down), (v_w_gate, v_w_up, v_w_down), gradients, strict=True)
    ]
    return tuple(one[which] for which in range(3) for one in new)
```

```python
import jax
import jax.numpy as jnp
from jax import lax
from jax.experimental import pallas as pl
from jax.experimental.pallas import tpu as pltpu
from jax.sharding import PartitionSpec as P

F32, BF16 = jnp.float32, jnp.bfloat16
MESH = pl.DeviceIdType.MESH
TOKENS, D, HALF, PART = 1024, 512, 4096, 1024
PAIR, STEP = 2 * TOKENS, 256
MIB = 2**20


def nt(a, b):
    return lax.dot_general(a, b, (((1,), (1,)), ((), ())), preferred_element_type=F32)


def nn(a, b):
    return jnp.dot(a, b, preferred_element_type=F32)


def scaled(wide):
    return lax.rsqrt(jnp.mean(wide * wide, -1, keepdims=True) + 1e-6)


def turned(a):
    return a.astype(F32).T.astype(BF16)


def blocks(body):
    def one(b, _):
        body(pl.ds(pl.multiple_of(b * STEP, STEP), STEP), pl.ds(pl.multiple_of((b * STEP + TOKENS) % PAIR, STEP), STEP))
        return 0

    lax.fori_loop(0, PAIR // STEP, one, 0)


def places():
    me, r = lax.axis_index("dp"), lax.axis_index("rep")
    c, z, y = me % 2, me // 2 % 4, me // 8
    row = [(r, y * 8 + (z + k) % 4 * 2 + c) for k in range(4)]
    return me, r, c, z, y, row, (r, (1 - y) * 8 + z * 2 + c), (r, me // 2 * 2 + 1 - c)


def greet(peers):
    barrier = pltpu.get_barrier_semaphore()
    for peer in peers:
        pl.semaphore_signal(barrier, inc=1, device_id=peer, device_id_type=MESH)
    pl.semaphore_wait(barrier, len(peers))


def remote(src, dst, send_sem, recv_sem, to):
    return pltpu.make_async_remote_copy(src_ref=src, dst_ref=dst, send_sem=send_sem, recv_sem=recv_sem, device_id=to, device_id_type=MESH)


def gather_kernel(
    wt, sd, x, dy, wgu, wd, out_h1, out_a0, out_a1, out_at0, out_at1, out_dy, out_dyt,
    sgu, vg, vu, vd, acc, got, h, a, at, h1, a1, at1, dys, dyt, send_sem, recv_sem, own_sem, load_sem, pair_sem, out_sem,
):
    me, r, c, z, y, row, across, partner = places()
    chip, other = me // 2, (1 - r, me)
    greet(row[1:] + [across, other, partner])

    mine, theirs = pl.ds(0, TOKENS), pl.ds(TOKENS, TOKENS)
    swaps = [(wt.at[1 - c], sgu.at[:, :, c]), (x, h.at[theirs]), (dy, dys.at[theirs])]
    swaps = [remote(src, dst, pair_sem.at[0, i], pair_sem.at[1, i], partner) for i, (src, dst) in enumerate(swaps)]
    stays = [(wt.at[c], sgu.at[:, :, c]), (x, h.at[mine]), (dy, dys.at[mine])]
    stays = [pltpu.make_async_copy(src, dst, load_sem.at[i]) for i, (src, dst) in enumerate(stays)]
    for one in swaps + stays:
        one.start()

    def place(n, i, chip, half):
        ref = wd.at[n, chip] if i == 1 else wgu.at[n, 1 - i // 2, chip]
        return ref if i == 2 else ref.at[half]

    def source(n, i):
        ref = sd.at[n] if i == 1 else sgu.at[n, 1 - i // 2]
        return ref if i == 2 else ref.at[r]

    def origin(slot):
        return (y if slot < 3 else 1 - y) * 4 + (z + (3 if slot < 3 else 7) - slot) % 4

    started = []

    def start(j, src, dst, slot, to):
        one = remote(src, dst, send_sem.at[j * 14 + slot], recv_sem.at[j * 14 + slot], to)
        one.start()
        started.append(one)

    def arrived(j, slot):
        n, i = divmod(j, 3)
        block = place(n, i, origin(slot % 7), 1 - r if slot > 6 else r)
        remote(block, block, send_sem.at[j * 14 + slot], recv_sem.at[j * 14 + slot], other).wait_recv()
        return block

    def begin(j):
        n, i = divmod(j, 3)
        for k in (1, 3, 2):
            start(j, source(n, i), place(n, i, chip, r), k - 1, row[k])

    def own_over_y(j):
        n, i = divmod(j, 3)
        start(j, source(n, i), place(n, i, chip, r), 3, across)

    def relay(j, slot):
        block = arrived(j, slot)
        if slot < 3:
            start(j, block, block, 4 + slot, across)
        if j % 3 < 2:
            start(j, block, block, 7 + slot, other)

    begin(1)
    own_over_y(1)
    swaps[0].wait()
    stays[0].wait()
    owns = []
    for n in range(2):
        for i, (ref, to) in enumerate(((sgu.at[n, 0], wgu.at[n, 0]), (sgu.at[n, 1], wgu.at[n, 1]), (sd.at[n], wd.at[n]))):
            owns.append(pltpu.make_async_copy(ref, to.at[chip], own_sem.at[3 * n + i]))
            owns[-1].start()
    begin(0)
    begin(2)

    saved = []

    def save(src, dst):
        saved.append(pltpu.make_async_copy(src, dst, out_sem.at[len(saved)]))
        saved[-1].start()

    def first_norm():
        for one in swaps[1:] + stays[1:]:
            one.wait()

        def body(rows, _):
            wide = h[rows, :].astype(F32)
            normed = (wide * scaled(wide)).astype(BF16)
            a[rows, :] = normed
            at[:, rows] = turned(normed)
            dyt[:, rows] = turned(dys[rows, :])

        blocks(body)
        save(a, out_a0)
        save(at, out_at0)
        save(dys, out_dy)
        save(dyt, out_dyt)

    def from_row(j):
        for slot in (0, 2, 1):
            relay(j, slot)

    def from_across(j):
        for slot in (3, 4, 6, 5):
            relay(j, slot)

    from_row(1)
    own_over_y(0)
    begin(4)
    first_norm()
    from_row(0)
    from_across(1)
    own_over_y(2)
    begin(3)
    from_row(2)
    begin(5)
    from_across(0)
    own_over_y(4)
    from_across(2)
    for one in owns:
        one.wait()
    for j in (1, 0):
        for slot in range(7, 14):
            arrived(j, slot)
    loads = [(wgu.at[0, 0], vg), (wgu.at[0, 1], vu), (wd.at[0], vd)]
    loads = [pltpu.make_async_copy(src, dst, load_sem.at[i]) for i, (src, dst) in enumerate(loads)]
    for one in loads:
        one.start()
    from_row(4)
    own_over_y(3)
    for one in loads:
        one.wait()

    def forward(t):
        cols = slice(t * D, t * D + D)

        def body(b, _):
            rows = pl.ds(pl.multiple_of(b * D, D), D)
            gate = nn(a[rows, :], vg[:, :, :, cols].reshape(D, D))
            up = nn(a[rows, :], vu[:, :, :, cols].reshape(D, D))
            part = nn((gate * jax.nn.sigmoid(gate) * up).astype(BF16), vd[t].reshape(D, D))
            acc[rows, :] = acc[rows, :] + part if t else part
            return 0

        lax.fori_loop(0, PAIR // D, body, 0)

    later = [lambda: from_row(3), lambda: from_across(4), lambda: own_over_y(5), lambda: from_across(3)]
    for t in range(8):
        forward(t)
        if t % 2:
            later[t // 2]()
    swap = remote(acc, got, pair_sem.at[0, 3], pair_sem.at[1, 3], partner)
    swap.start()
    relay(5, 0)
    swap.wait()

    def second_norm(rows, theirs):
        state = h[rows, :] + (acc[rows, :] + got[theirs, :]).astype(BF16)
        wide = state.astype(F32)
        normed = (wide * scaled(wide)).astype(BF16)
        h1[rows, :] = state
        a1[rows, :] = normed
        at1[:, rows] = turned(normed)

    blocks(second_norm)
    save(h1, out_h1)
    save(a1, out_a1)
    save(at1, out_at1)
    relay(5, 2)
    relay(5, 1)
    from_across(5)
    for j in (4, 3):
        for slot in range(7, 14):
            arrived(j, slot)
    for one in saved:
        one.wait()
    for one in started:
        one.wait_send()


def shape(*dims, dtype=BF16):
    return jax.ShapeDtypeStruct(dims, dtype)


ANY, VMEM = pl.BlockSpec(memory_space=pl.ANY), pl.BlockSpec(memory_space=pltpu.VMEM)


def bf(*dims):
    return pltpu.VMEM(dims, BF16)


def wide(*dims):
    return pltpu.VMEM(dims, F32)


def dma(*dims):
    return pltpu.SemaphoreType.DMA(dims)


def gather(wt, sd, x, dy):
    rows, cols = (PAIR, D), (D, PAIR)
    return pl.pallas_call(
        gather_kernel,
        out_shape=(shape(2, 2, 8, 2, 32, HALF), shape(2, 8, 2, 256, D)) + tuple(shape(*s) for s in (rows, rows, rows, cols, cols, rows, cols)),
        in_specs=[VMEM] * 4,
        out_specs=(ANY,) * 9,
        scratch_shapes=[
            bf(2, 2, 2, 32, HALF), bf(8, 2, 32, HALF), bf(8, 2, 32, HALF), bf(8, 2, 256, D), wide(*rows), wide(*rows),
            bf(*rows), bf(*rows), bf(*cols), bf(*rows), bf(*rows), bf(*cols), bf(*rows), bf(*cols),
            dma(84), dma(84), dma(6), dma(3), dma(2, 4), dma(7),
        ],
        compiler_params=pltpu.CompilerParams(collective_id=0, has_side_effects=True, vmem_limit_bytes=60 * MIB),
        name="gather_forward",
    )(wt, sd, x, dy)


def backward_kernel(
    wgu, wd, a0, a1, at0, at1, dy, dyt, h1, out_d, out_g, square, from_y_d, from_y_g, from_z_d, from_z_g,
    a, at, by_h, by_ht, by_a, got, act, by_gate, by_up, vgu, vd, unit_d, unit_g, stage_yd, stage_yg, sent_d, sent_g, own_d, own_g,
    stage_zd, stage_zg, whole, sums, y_send, y_recv, z_send, z_recv, stage_sem, load_sem, w_sem, pair_sem, core_sem, sum_sem,
):
    me, r, c, z, y, row, across, partner = places()
    greet(row[1:] + [across, partner])

    def trio(d, g):
        return [d, g.at[0], g.at[1]]

    unit, from_y, from_z, stage_y = trio(unit_d, unit_g), trio(from_y_d, from_y_g), trio(from_z_d, from_z_g), trio(stage_yd, stage_yg)
    stage_z, sent, own = trio(stage_zd, stage_zg), trio(sent_d, sent_g), trio(own_d, own_g)

    def over_y(k, i):
        src = unit[i].at[k % 2, pl.ds((1 - y) * 4, 4)]
        return remote(src, from_y[i].at[k], y_send.at[k * 3 + i], y_recv.at[k * 3 + i], across)

    def over_z(k, i, hop):
        at = (k * 3 + i) * 3 + hop - 1
        return remote(sent[i].at[k % 2, hop - 1], from_z[i].at[k, hop - 1], z_send.at[at], z_recv.at[at], row[hop])

    def over_cores(k, i):
        at = (i - 1) * 8 + k
        return remote(whole.at[i - 1, k, 1 - c], out_g.at[i - 1, k, c], core_sem.at[0, at], core_sem.at[1, at], partner)

    def stage_of_y(k, i):
        return pltpu.make_async_copy(from_y[i].at[k], stage_y[i], stage_sem.at[i])

    def stage_of_z(k, i):
        return pltpu.make_async_copy(from_z[i].at[k], stage_z[i], stage_sem.at[3 + i])

    def fetch_y(k, i):
        over_y(k, i).wait_recv()
        stage_of_y(k, i).start()

    def add_y(k, i):
        stage_of_y(k, i).wait()
        over_y(k, i).wait_send()
        for hop in (2, 1, 3, 0):
            to = (z + hop) % 4
            total = unit[i][k % 2, y * 4 + to].astype(F32) + stage_y[i][to].astype(F32)
            if hop:
                sent[i][k % 2, hop - 1] = total.astype(BF16)
                over_z(k, i, hop).start()
            else:
                own[i][k % 2] = total

    def fetch_z(k, i):
        for hop in (1, 3, 2):
            over_z(k, i, hop).wait()
        stage_of_z(k, i).start()

    def add_z(k, i):
        stage_of_z(k, i).wait()
        total = own[i][k % 2]
        for hop in range(3):
            total = total + stage_z[i][hop].astype(F32)
        total = total.astype(BF16)
        if i:
            whole[i - 1, k] = total
            out_g[i - 1, k, c] = whole[i - 1, k, c]
            over_cores(k, i).start()
        else:
            out_d[k] = total
        g = total.astype(F32)
        g = jnp.sum((g * g).reshape(-1, 8, g.shape[-1]), 0)
        parts = [g[:, j : j + 128] for j in range(0, g.shape[-1], 128)]
        sums[0] += sum(parts[1:], parts[0])

    lags = ((add_y, 5), (fetch_y, 4), (add_z, 8), (fetch_z, 7))

    def advance(k, i, known):
        for step, lag in lags:
            back, which = divmod(i - lag, 3)

            @pl.when(known | (k + back >= 0))
            def _():
                step(k + back, which)

    def weights(n, q):
        slot, some = q % 2, pl.ds(pl.multiple_of(q * 128, 128), 128)
        copies = [pltpu.make_async_copy(wd.at[n, :, q // 2, pl.ds(pl.multiple_of(q % 2 * 128, 128), 128)], vd.at[slot], w_sem.at[slot, 8])]
        for j in range(8):
            src = wgu.at[n, :, :, :, :, pl.ds(pl.multiple_of(j * D + q * 128, 128), 128)]
            copies.append(pltpu.make_async_copy(src, vgu.at[slot, :, :, :, :, pl.ds(j * 128, 128)], w_sem.at[slot, j]))
        return copies

    def begin(copies):
        for one in copies:
            one.start()

    def finish(copies):
        for one in copies:
            one.wait()

    def fill(pairs):
        copies = [pltpu.make_async_copy(src, dst, load_sem.at[i]) for i, (src, dst) in enumerate(pairs)]
        begin(copies)
        return copies

    sums[0] = jnp.zeros_like(sums[0])
    loads = fill([(a1, a), (dy, by_h), (at1, at), (dyt, by_ht)])
    begin(weights(1, me * 0))
    finish(loads)

    def layer(n):
        def part(q, _):
            k, slot = (1 - n) * 4 + q, q % 2
            finish(weights(n, q))
            pl.when(q < 3)(lambda: begin(weights(n, q + 1)))
            if n:
                pl.when(q == 3)(lambda: begin(weights(0, q - 3)))

            def body(rows, _):
                gate_w, up_w = (vgu[slot, j].reshape(D, PART) for j in range(2))
                gate, up = nn(a[rows, :], gate_w), nn(a[rows, :], up_w)
                by_act = nt(by_h[rows, :], vd[slot].reshape(PART, D)).astype(BF16).astype(F32)
                sig = jax.nn.sigmoid(gate)
                silu = gate * sig
                act[rows, :] = (silu * up).astype(BF16)
                g = (by_act * up * (sig + silu * (1.0 - sig))).astype(BF16)
                u = (by_act * silu).astype(BF16)
                by_gate[rows, :] = g
                by_up[rows, :] = u
                if n:
                    total = nt(g, gate_w) + nt(u, up_w)

                    @pl.when(q == 0)
                    def _():
                        by_a[rows, :] = total

                    @pl.when(q > 0)
                    def _():
                        by_a[rows, :] += total

            blocks(body)
            for i, (left, right) in enumerate(((by_ht, act), (at, by_gate), (at, by_up))):

                def columns(j, _):
                    cols = pl.ds(pl.multiple_of(j * STEP, STEP), STEP)
                    g = nn(left[...], right[:, cols]).astype(BF16)
                    if i:
                        unit_g[i - 1, k % 2, :, :, :, cols] = g.reshape(8, 2, 32, STEP)
                    else:
                        unit_d[k % 2, 2 * j] = g[:, :128]
                        unit_d[k % 2, 2 * j + 1] = g[:, 128:]
                    return 0

                lax.fori_loop(0, PART // STEP, columns, 0)
                over_y(k, i).start()
                advance(k, i, False)
            return 0

        lax.fori_loop(0, 4, part, 0)

    layer(1)
    swap = remote(by_a, got, pair_sem.at[0], pair_sem.at[1], partner)
    swap.start()
    loads = fill([(a0, a), (at0, at)])
    swap.wait()

    def between(rows, theirs):
        g = (by_a[rows, :] + got[theirs, :]).astype(BF16).astype(F32)
        state = h1[rows, :].astype(F32)
        scale = scaled(state)
        inner = jnp.mean(g * state, -1, keepdims=True)
        total = by_h[rows, :] + (g * scale - state * (scale * scale * scale * inner)).astype(BF16)
        by_h[rows, :] = total
        by_ht[:, rows] = turned(total)

    blocks(between)
    finish(loads)
    layer(0)
    for s in range(24, 32):
        for step, lag in lags:
            if s - lag < 24:
                step(*divmod(s - lag, 3))

    def share(src, at, to):
        one = remote(sums.at[src], sums.at[at], sum_sem.at[0, at], sum_sem.at[1, at], to)
        one.start()
        return one

    share(0, 3, partner).wait()
    sums[1] = sums[0] + sums[3]
    share(1, 4, across).wait()
    sums[2] = sums[1] + sums[4]
    finish([share(2, 4 + hop, row[hop]) for hop in (1, 2, 3)])
    square[...] = sums[2] + sums[5] + sums[6] + sums[7]
    for i in (1, 2):
        for k in range(8):
            over_cores(k, i).wait()


def backward(wgu, wd, a0, a1, at0, at1, dy, dyt, h1):
    rows, cols, g, d = (PAIR, D), (D, PAIR), (2, 32, PART), (D, 128)
    part = (PAIR, PART)
    return pl.pallas_call(
        backward_kernel,
        out_shape=(
            shape(8, *d), shape(2, 8, *g), shape(8, 128, dtype=F32), shape(8, 4, *d), shape(2, 8, 4, *g), shape(8, 3, *d), shape(2, 8, 3, *g),
        ),
        in_specs=[ANY] * 8 + [VMEM],
        out_specs=(VMEM,) * 3 + (ANY,) * 4,
        scratch_shapes=[
            bf(*rows), bf(*cols), bf(*rows), bf(*cols), wide(*rows), wide(*rows), bf(*part), bf(*part), bf(*part),
            bf(2, 2, 8, 2, 32, PART), bf(2, 8, 128, D), bf(2, 8, *d), bf(2, 2, 8, *g), bf(4, *d), bf(2, 4, *g), bf(2, 3, *d), bf(2, 2, 3, *g),
            wide(2, *d), wide(2, 2, *g), bf(3, *d), bf(2, 3, *g), bf(2, 8, *g), wide(8, 8, 128),
            dma(24), dma(24), dma(72), dma(72), dma(6), dma(4), dma(2, 9), dma(2), dma(2, 16), dma(2, 8),
        ],
        compiler_params=pltpu.CompilerParams(collective_id=1, has_side_effects=True, vmem_limit_bytes=63 * MIB),
        name="backward_sum",
    )(wgu, wd, a0, a1, at0, at1, dy, dyt, h1)


def adamw(w, m, v, g):
    m = 0.9 * m + 0.1 * g
    v = 0.95 * v + 0.05 * g * g
    step = m * lax.rsqrt(v + 1e-8) + 0.1 * w
    return (w - 0.02 * step).astype(BF16), m, v


def update_kernel(count, square, by_d, by_gate, by_up, *refs):
    olds, news = refs[:9], refs[9:]
    factor = jnp.minimum(1.0, 0.5 * lax.rsqrt(jnp.sum(square[...]) / count + 1e-30))

    def columns(g):
        pieces = [(j, core, q) for j in range(2) for core in range(2) for q in range(4)]
        return jnp.concatenate([g[0, q, core, :, j * 128 : j * 128 + 128] for j, core, q in pieces], 1)

    for i, g in enumerate((columns(by_gate), columns(by_up), by_d[0].astype(F32).T)):
        w, m, v = (ref[0] for ref in olds[i::3])
        for ref, one in zip(news[i::3], adamw(w.astype(F32), m, v, g.astype(F32) * factor), strict=True):
            ref[0] = one


def update(square, by_d, by_g, arrays):
    grid, layers = (arrays[0].shape[0], 4), arrays[0].shape[0]
    up = pl.BlockSpec((1, 32, 8192 // 4), lambda n, s: (n, 0, s))
    down = pl.BlockSpec((1, 128, D), lambda n, s: (n, s, 0))
    own = [up, up, down] * 3
    g = [pl.BlockSpec((1, 4, 2, 32, STEP), lambda n, s, i=i: (i, 1 - n, 0, 0, s)) for i in range(2)]
    return pl.pallas_call(
        lambda *refs: update_kernel(16 * sum(w.size for w in arrays[:3]), *refs),
        grid=grid,
        out_shape=tuple(jax.ShapeDtypeStruct(w.shape, w.dtype) for w in arrays),
        in_specs=[pl.BlockSpec((8, 128), lambda n, s: (0, 0)), pl.BlockSpec((1, D, 128), lambda n, s: ((1 - n) * 4 + s, 0, 0)), *g, *own],
        out_specs=tuple(own),
        name="update",
    )(square, by_d, by_g, by_g, *arrays)


def solution(mesh):
    def step(x, dy, *arrays):
        w_gate, w_up, w_down = arrays[:3]
        layers = w_gate.shape[0]
        wt = jnp.stack([w_gate, w_up], 1).reshape(layers, 2, 32, 8, 2, D).transpose(4, 0, 1, 2, 3, 5).reshape(2, layers, 2, 32, HALF)
        wgu, wd, h1, *rest = gather(wt, w_down.reshape(layers, 2, 256, D), x[0], dy[0])
        by_d, by_g, square = backward(wgu, wd, *rest, h1)[:3]
        return tuple(update(square, by_d, by_g, arrays))

    states, cut = P(("rep", "dp"), None, None), P(None, "dp", None)
    return jax.shard_map(
        step,
        mesh=mesh,
        in_specs=(states, states) + (cut,) * 9,
        out_specs=(P("rep", "dp", None),) * 9,
        check_vma=False,
    )
```

```python
import jax
import jax.numpy as jnp
from jax import lax
from jax.experimental import pallas as pl
from jax.experimental.pallas import tpu as pltpu
from jax.sharding import PartitionSpec as P

F32, BF16 = jnp.float32, jnp.bfloat16
MESH = pl.DeviceIdType.MESH
TOKENS, D, HALF, PART = 1024, 512, 4096, 1024
PAIR, STEP = 2 * TOKENS, 256
MIB = 2**20


def nt(a, b):
    return lax.dot_general(a, b, (((1,), (1,)), ((), ())), preferred_element_type=F32)


def nn(a, b):
    return jnp.dot(a, b, preferred_element_type=F32)


def scaled(wide):
    return lax.rsqrt(jnp.mean(wide * wide, -1, keepdims=True) + 1e-6)


def turned(a):
    return a.astype(F32).T.astype(BF16)


def blocks(body, low=0, high=PAIR // STEP):
    def one(b, _):
        body(pl.ds(pl.multiple_of(b * STEP, STEP), STEP), pl.ds(pl.multiple_of((b * STEP + TOKENS) % PAIR, STEP), STEP))
        return 0

    lax.fori_loop(low, high, one, 0)


def places():
    me, r = lax.axis_index("dp"), lax.axis_index("rep")
    c, z, y = me % 2, me // 2 % 4, me // 8
    row = [(r, y * 8 + (z + k) % 4 * 2 + c) for k in range(4)]
    return me, r, c, z, y, row, (r, (1 - y) * 8 + z * 2 + c), (r, me // 2 * 2 + 1 - c)


def greet(peers):
    barrier = pltpu.get_barrier_semaphore()
    for peer in peers:
        pl.semaphore_signal(barrier, inc=1, device_id=peer, device_id_type=MESH)
    pl.semaphore_wait(barrier, len(peers))


def remote(src, dst, send_sem, recv_sem, to):
    return pltpu.make_async_remote_copy(src_ref=src, dst_ref=dst, send_sem=send_sem, recv_sem=recv_sem, device_id=to, device_id_type=MESH)


def gather_kernel(
    w_gate, w_up, sd, x, dy, wgu, wd, out_h1, out_a0, out_a1, out_at0, out_at1, out_dy, out_dyt,
    give, sgu, vg, vu, vd, acc, got, h, a, at, h1, a1, at1, dys, dyt, send_sem, recv_sem, own_sem, load_sem, pair_sem, out_sem,
):
    me, r, c, z, y, row, across, partner = places()
    chip, other = me // 2, (1 - r, me)

    def split(j, _):
        to, own, its = (pl.ds(pl.multiple_of(at * D, D), D) for at in (j, 2 * j + c, 2 * j + 1 - c))
        for n in range(2):
            for m, w in enumerate((w_gate, w_up)):
                give[n, m, :, to] = w[n, :, its]
                sgu[n, m, c, :, to] = w[n, :, own]
        return 0

    lax.fori_loop(0, 8, split, 0)
    greet(row[1:] + [across, other, partner])

    mine, theirs = pl.ds(0, TOKENS), pl.ds(TOKENS, TOKENS)
    swaps = [(give, sgu.at[:, :, c]), (x, h.at[theirs]), (dy, dys.at[theirs])]
    swaps = [remote(src, dst, pair_sem.at[0, i], pair_sem.at[1, i], partner) for i, (src, dst) in enumerate(swaps)]
    stays = [(x, h.at[mine]), (dy, dys.at[mine])]
    stays = [pltpu.make_async_copy(src, dst, load_sem.at[i]) for i, (src, dst) in enumerate(stays)]
    for one in swaps + stays:
        one.start()

    def gate(ref, i):
        return ref.at[0] if i == 2 else ref.at[1, pl.ds(i * 16 - 48, 16)]

    def place(n, i, chip, half):
        if i > 1:
            return gate(wgu.at[n, 0, chip], i)
        return wd.at[n, chip, half] if i else wgu.at[n, 1, chip, half]

    def source(n, i):
        if i > 1:
            return gate(sgu.at[n, 0], i)
        return sd.at[n, r] if i else sgu.at[n, 1, r]

    def origin(slot):
        return (y if slot < 3 else 1 - y) * 4 + (z + (3 if slot < 3 else 7) - slot) % 4

    started = []

    def start(j, src, dst, slot, to):
        one = remote(src, dst, send_sem.at[j * 14 + slot], recv_sem.at[j * 14 + slot], to)
        one.start()
        started.append(one)

    def arrived(j, slot):
        n, i = divmod(j, 5)
        block = place(n, i, origin(slot % 7), 1 - r if slot > 6 else r)
        remote(block, block, send_sem.at[j * 14 + slot], recv_sem.at[j * 14 + slot], other).wait_recv()
        return block

    def begin(j):
        n, i = divmod(j, 5)
        for k in (1, 3, 2):
            start(j, source(n, i), place(n, i, chip, r), k - 1, row[k])

    def own_over_y(j):
        n, i = divmod(j, 5)
        start(j, source(n, i), place(n, i, chip, r), 3, across)

    def ahead(j):
        begin(j)
        own_over_y(j)

    def relay(j, slot):
        block = arrived(j, slot)
        if slot < 3:
            start(j, block, block, 4 + slot, across)
        if j % 5 < 2:
            start(j, block, block, 7 + slot, other)

    ahead(1)
    swaps[0].wait()
    owns = []
    for n in range(2):
        for i, (ref, to) in enumerate(((sgu.at[n, 0], wgu.at[n, 0]), (sgu.at[n, 1], wgu.at[n, 1]), (sd.at[n], wd.at[n]))):
            owns.append(pltpu.make_async_copy(ref, to.at[chip], own_sem.at[3 * n + i]))
            owns[-1].start()
    ahead(0)
    for j in (2, 3, 4):
        own_over_y(j)

    saved = []

    def save(src, dst):
        saved.append(pltpu.make_async_copy(src, dst, out_sem.at[len(saved)]))
        saved[-1].start()

    def first_norm():
        for one in swaps[1:] + stays:
            one.wait()

        def body(rows, _):
            wide = h[rows, :].astype(F32)
            normed = (wide * scaled(wide)).astype(BF16)
            a[rows, :] = normed
            at[:, rows] = turned(normed)
            dyt[:, rows] = turned(dys[rows, :])

        blocks(body)
        save(a, out_a0)
        save(at, out_at0)
        save(dys, out_dy)
        save(dyt, out_dyt)

    def from_row(j):
        for slot in (0, 2, 1):
            relay(j, slot)

    def from_across(j):
        for slot in (3, 4, 6, 5):
            relay(j, slot)

    from_row(1)
    begin(2)
    first_norm()
    from_row(0)
    begin(3)
    begin(4)
    from_across(1)
    from_row(2)
    ahead(6)
    from_across(0)
    from_row(3)
    from_row(4)
    ahead(5)
    from_across(2)
    from_across(3)
    from_across(4)
    for one in owns:
        one.wait()
    for j in (1, 0):
        for slot in range(7, 14):
            arrived(j, slot)
    loads = [(wgu.at[0, 0], vg), (wgu.at[0, 1], vu), (wd.at[0], vd)]
    loads = [pltpu.make_async_copy(src, dst, load_sem.at[i]) for i, (src, dst) in enumerate(loads)]
    for one in loads:
        one.start()
    from_row(6)
    ahead(7)
    for one in loads:
        one.wait()

    def forward(t):
        cols = slice(t * D, t * D + D)

        def body(b, _):
            rows = pl.ds(pl.multiple_of(b * D, D), D)
            gate = nn(a[rows, :], vg[:, :, :, cols].reshape(D, D))
            up = nn(a[rows, :], vu[:, :, :, cols].reshape(D, D))
            part = nn((gate * jax.nn.sigmoid(gate) * up).astype(BF16), vd[t].reshape(D, D))
            acc[rows, :] = acc[rows, :] + part if t else part
            return 0

        lax.fori_loop(0, PAIR // D, body, 0)

    later = {1: (from_row, 5), 2: (ahead, 8), 3: (from_across, 6), 5: (from_across, 5), 6: (from_row, 7)}
    for t in range(8):
        forward(t)
        if t in later:
            later[t][0](later[t][1])
    ahead(9)
    swap = remote(acc, got, pair_sem.at[0, 3], pair_sem.at[1, 3], partner)
    swap.start()
    from_across(7)
    swap.wait()

    def second_norm(rows, theirs):
        state = h[rows, :] + (acc[rows, :] + got[theirs, :]).astype(BF16)
        wide = state.astype(F32)
        normed = (wide * scaled(wide)).astype(BF16)
        h1[rows, :] = state
        a1[rows, :] = normed
        at1[:, rows] = turned(normed)

    blocks(second_norm)
    save(h1, out_h1)
    save(a1, out_a1)
    save(at1, out_at1)
    from_row(8)
    from_row(9)
    from_across(8)
    from_across(9)
    for j in (6, 5):
        for slot in range(7, 14):
            arrived(j, slot)
    for one in saved:
        one.wait()
    for one in started:
        one.wait_send()


def shape(*dims, dtype=BF16):
    return jax.ShapeDtypeStruct(dims, dtype)


ANY, VMEM = pl.BlockSpec(memory_space=pl.ANY), pl.BlockSpec(memory_space=pltpu.VMEM)


def bf(*dims):
    return pltpu.VMEM(dims, BF16)


def wide(*dims):
    return pltpu.VMEM(dims, F32)


def dma(*dims):
    return pltpu.SemaphoreType.DMA(dims)


def gather(*args):
    rows, cols = (PAIR, D), (D, PAIR)
    return pl.pallas_call(
        gather_kernel,
        out_shape=(shape(2, 2, 8, 2, 32, HALF), shape(2, 8, 2, 256, D)) + tuple(shape(*s) for s in (rows, rows, rows, cols, cols, rows, cols)),
        in_specs=[VMEM] * 5,
        out_specs=(ANY,) * 9,
        scratch_shapes=[
            bf(2, 2, 32, HALF), bf(2, 2, 2, 32, HALF), bf(8, 2, 32, HALF), bf(8, 2, 32, HALF), bf(8, 2, 256, D), wide(*rows), wide(*rows),
            bf(*rows), bf(*rows), bf(*cols), bf(*rows), bf(*rows), bf(*cols), bf(*rows), bf(*cols),
            dma(140), dma(140), dma(6), dma(3), dma(2, 4), dma(7),
        ],
        compiler_params=pltpu.CompilerParams(collective_id=0, has_side_effects=True, vmem_limit_bytes=60 * MIB),
        name="gather_forward",
    )(*args)


def backward_kernel(
    wgu, wd, a0, a1, at0, at1, dy, dyt, h1, out_d, out_g, square, from_y_d, from_y_g, from_z_d, from_z_g,
    a, at, by_h, by_ht, by_a, got, act, by_gate, by_up, vgu, vd, unit_d, unit_g, stage_yd, stage_yg, sent_d, sent_g, own_d, own_g,
    stage_zd, stage_zg, whole, sums, y_send, y_recv, z_send, z_recv, stage_sem, load_sem, w_sem, pair_sem, core_sem, sum_sem,
):
    me, r, c, z, y, row, across, partner = places()

    def trio(d, g):
        return [d, g.at[0], g.at[1]]

    unit, from_y, from_z, stage_y = trio(unit_d, unit_g), trio(from_y_d, from_y_g), trio(from_z_d, from_z_g), trio(stage_yd, stage_yg)
    stage_z, sent, own = trio(stage_zd, stage_zg), trio(sent_d, sent_g), trio(own_d, own_g)

    def over_y(k, i):
        src = unit[i].at[k % 2, pl.ds((1 - y) * 4, 4)]
        return remote(src, from_y[i].at[k], y_send.at[k * 3 + i], y_recv.at[k * 3 + i], across)

    def over_z(k, i, hop):
        at = (k * 3 + i) * 3 + hop - 1
        return remote(sent[i].at[k % 2, hop - 1], from_z[i].at[k, hop - 1], z_send.at[at], z_recv.at[at], row[hop])

    def over_cores(k, i):
        at = (i - 1) * 8 + k
        return remote(whole.at[i - 1, k, 1 - c], out_g.at[i - 1, k, c], core_sem.at[0, at], core_sem.at[1, at], partner)

    def stage_of_y(k, i):
        return pltpu.make_async_copy(from_y[i].at[k], stage_y[i], stage_sem.at[i])

    def stage_of_z(k, i):
        return pltpu.make_async_copy(from_z[i].at[k], stage_z[i], stage_sem.at[3 + i])

    def fetch_y(k, i):
        over_y(k, i).wait_recv()
        stage_of_y(k, i).start()

    def add_y(k, i):
        stage_of_y(k, i).wait()
        over_y(k, i).wait_send()
        for hop in (2, 1, 3, 0):
            to = (z + hop) % 4
            total = unit[i][k % 2, y * 4 + to].astype(F32) + stage_y[i][to].astype(F32)
            if hop:
                sent[i][k % 2, hop - 1] = total.astype(BF16)
                over_z(k, i, hop).start()
            else:
                own[i][k % 2] = total

    def fetch_z(k, i):
        for hop in (1, 3, 2):
            over_z(k, i, hop).wait()
        stage_of_z(k, i).start()

    def add_z(k, i):
        stage_of_z(k, i).wait()
        total = own[i][k % 2]
        for hop in range(3):
            total = total + stage_z[i][hop].astype(F32)
        total = total.astype(BF16)
        if i:
            whole[i - 1, k] = total
            out_g[i - 1, k, c] = whole[i - 1, k, c]
            over_cores(k, i).start()
        else:
            out_d[k] = total
        g = total.astype(F32)
        g = jnp.sum((g * g).reshape(-1, 8, g.shape[-1]), 0)
        parts = [g[:, j : j + 128] for j in range(0, g.shape[-1], 128)]
        sums[0] += sum(parts[1:], parts[0])

    lags = ((add_y, 4), (fetch_y, 3), (add_z, 7), (fetch_z, 6))

    def advance(k, i, known):
        for step, lag in lags:
            back, which = divmod(i - lag, 3)

            @pl.when(known | (k + back >= 0))
            def _():
                step(k + back, which)

    def weights(n, q):
        slot, some = q % 2, pl.ds(pl.multiple_of(q * 128, 128), 128)
        copies = [pltpu.make_async_copy(wd.at[n, :, q // 2, pl.ds(pl.multiple_of(q % 2 * 128, 128), 128)], vd.at[slot], w_sem.at[slot, 8])]
        for j in range(8):
            src = wgu.at[n, :, :, :, :, pl.ds(pl.multiple_of(j * D + q * 128, 128), 128)]
            copies.append(pltpu.make_async_copy(src, vgu.at[slot, :, :, :, :, pl.ds(j * 128, 128)], w_sem.at[slot, j]))
        return copies

    def begin(copies):
        for one in copies:
            one.start()

    def finish(copies):
        for one in copies:
            one.wait()

    def fill(pairs):
        copies = [pltpu.make_async_copy(src, dst, load_sem.at[i]) for i, (src, dst) in enumerate(pairs)]
        begin(copies)
        return copies

    sums[0] = jnp.zeros_like(sums[0])
    loads = fill([(a1, a), (dy, by_h), (at1, at), (dyt, by_ht)])
    begin(weights(1, me * 0))
    greet(row[1:] + [across, partner])
    finish(loads)

    def layer(n):
        def part(q, _):
            k, slot = (1 - n) * 4 + q, q % 2
            finish(weights(n, q))
            pl.when(q < 3)(lambda: begin(weights(n, q + 1)))
            if n:
                pl.when(q == 3)(lambda: begin(weights(0, q - 3)))

            def body(rows, _):
                gate_w, up_w = (vgu[slot, j].reshape(D, PART) for j in range(2))
                gate, up = nn(a[rows, :], gate_w), nn(a[rows, :], up_w)
                by_act = nt(by_h[rows, :], vd[slot].reshape(PART, D)).astype(BF16).astype(F32)
                sig = jax.nn.sigmoid(gate)
                silu = gate * sig
                act[rows, :] = (silu * up).astype(BF16)
                g = (by_act * up * (sig + silu * (1.0 - sig))).astype(BF16)
                u = (by_act * silu).astype(BF16)
                by_gate[rows, :] = g
                by_up[rows, :] = u
                if n:
                    total = nt(g, gate_w) + nt(u, up_w)

                    @pl.when(q == 0)
                    def _():
                        by_a[rows, :] = total

                    @pl.when(q > 0)
                    def _():
                        by_a[rows, :] += total

            blocks(body, 0, 4)
            advance(k, 0, False)
            blocks(body, 4)
            for i, (left, right) in enumerate(((by_ht, act), (at, by_gate), (at, by_up))):

                def columns(j, _):
                    cols = pl.ds(pl.multiple_of(j * STEP, STEP), STEP)
                    g = nn(left[...], right[:, cols]).astype(BF16)
                    if i:
                        unit_g[i - 1, k % 2, :, :, :, cols] = g.reshape(8, 2, 32, STEP)
                    else:
                        unit_d[k % 2, 2 * j] = g[:, :128]
                        unit_d[k % 2, 2 * j + 1] = g[:, 128:]
                    return 0

                lax.fori_loop(0, PART // STEP, columns, 0)
                over_y(k, i).start()
                if i != 1:
                    advance(k, 1 + i // 2, False)
            return 0

        lax.fori_loop(0, 4, part, 0)

    layer(1)
    swap = remote(by_a, got, pair_sem.at[0], pair_sem.at[1], partner)
    swap.start()
    loads = fill([(a0, a), (at0, at)])
    swap.wait()

    def between(rows, theirs):
        g = (by_a[rows, :] + got[theirs, :]).astype(BF16).astype(F32)
        state = h1[rows, :].astype(F32)
        scale = scaled(state)
        inner = jnp.mean(g * state, -1, keepdims=True)
        total = by_h[rows, :] + (g * scale - state * (scale * scale * scale * inner)).astype(BF16)
        by_h[rows, :] = total
        by_ht[:, rows] = turned(total)

    blocks(between)
    finish(loads)
    layer(0)
    for s in range(24, 31):
        for step, lag in lags:
            if s - lag < 24:
                step(*divmod(s - lag, 3))

    def share(src, at, to):
        one = remote(sums.at[src], sums.at[at], sum_sem.at[0, at], sum_sem.at[1, at], to)
        one.start()
        return one

    share(0, 3, partner).wait()
    sums[1] = sums[0] + sums[3]
    share(1, 4, across).wait()
    sums[2] = sums[1] + sums[4]
    finish([share(2, 4 + hop, row[hop]) for hop in (1, 2, 3)])
    square[...] = sums[2] + sums[5] + sums[6] + sums[7]
    for i in (1, 2):
        for k in range(8):
            over_cores(k, i).wait()


def backward(wgu, wd, a0, a1, at0, at1, dy, dyt, h1):
    rows, cols, g, d = (PAIR, D), (D, PAIR), (2, 32, PART), (D, 128)
    part = (PAIR, PART)
    return pl.pallas_call(
        backward_kernel,
        out_shape=(
            shape(8, *d), shape(2, 8, *g), shape(8, 128, dtype=F32), shape(8, 4, *d), shape(2, 8, 4, *g), shape(8, 3, *d), shape(2, 8, 3, *g),
        ),
        in_specs=[ANY] * 8 + [VMEM],
        out_specs=(VMEM,) * 3 + (ANY,) * 4,
        scratch_shapes=[
            bf(*rows), bf(*cols), bf(*rows), bf(*cols), wide(*rows), wide(*rows), bf(*part), bf(*part), bf(*part),
            bf(2, 2, 8, 2, 32, PART), bf(2, 8, 128, D), bf(2, 8, *d), bf(2, 2, 8, *g), bf(4, *d), bf(2, 4, *g), bf(2, 3, *d), bf(2, 2, 3, *g),
            wide(2, *d), wide(2, 2, *g), bf(3, *d), bf(2, 3, *g), bf(2, 8, *g), wide(8, 8, 128),
            dma(24), dma(24), dma(72), dma(72), dma(6), dma(4), dma(2, 9), dma(2), dma(2, 16), dma(2, 8),
        ],
        compiler_params=pltpu.CompilerParams(collective_id=1, has_side_effects=True, vmem_limit_bytes=63 * MIB),
        name="backward_sum",
    )(wgu, wd, a0, a1, at0, at1, dy, dyt, h1)


def adamw(w, m, v, g):
    m = 0.9 * m + 0.1 * g
    v = 0.95 * v + 0.05 * g * g
    step = m * lax.rsqrt(v + 1e-8) + 0.1 * w
    return (w - 0.02 * step).astype(BF16), m, v


def update_kernel(count, square, by_d, by_gate, by_up, *refs):
    olds, news = refs[:9], refs[9:]
    factor = jnp.minimum(1.0, 0.5 * lax.rsqrt(jnp.sum(square[...]) / count + 1e-30))

    def columns(g):
        pieces = [(j, core, q) for j in range(2) for core in range(2) for q in range(4)]
        return jnp.concatenate([g[0, q, core, :, j * 128 : j * 128 + 128] for j, core, q in pieces], 1)

    for i, g in enumerate((columns(by_gate), columns(by_up), by_d[0].astype(F32).T)):
        w, m, v = (ref[0] for ref in olds[i::3])
        for ref, one in zip(news[i::3], adamw(w.astype(F32), m, v, g.astype(F32) * factor), strict=True):
            ref[0] = one


def update(square, by_d, by_g, arrays):
    grid, layers = (arrays[0].shape[0], 4), arrays[0].shape[0]
    up = pl.BlockSpec((1, 32, 8192 // 4), lambda n, s: (n, 0, s))
    down = pl.BlockSpec((1, 128, D), lambda n, s: (n, s, 0))
    own = [up, up, down] * 3
    g = [pl.BlockSpec((1, 4, 2, 32, STEP), lambda n, s, i=i: (i, 1 - n, 0, 0, s)) for i in range(2)]
    return pl.pallas_call(
        lambda *refs: update_kernel(16 * sum(w.size for w in arrays[:3]), *refs),
        grid=grid,
        out_shape=tuple(jax.ShapeDtypeStruct(w.shape, w.dtype) for w in arrays),
        in_specs=[pl.BlockSpec((8, 128), lambda n, s: (0, 0)), pl.BlockSpec((1, D, 128), lambda n, s: ((1 - n) * 4 + s, 0, 0)), *g, *own],
        out_specs=tuple(own),
        name="update",
    )(square, by_d, by_g, by_g, *arrays)


def solution(mesh):
    def step(x, dy, *arrays):
        w_gate, w_up, w_down = arrays[:3]
        layers = w_gate.shape[0]
        wgu, wd, h1, *rest = gather(w_gate, w_up, w_down.reshape(layers, 2, 256, D), x[0], dy[0])
        by_d, by_g, square = backward(wgu, wd, *rest, h1)[:3]
        return tuple(update(square, by_d, by_g, arrays))

    states, cut = P(("rep", "dp"), None, None), P(None, "dp", None)
    return jax.shard_map(
        step,
        mesh=mesh,
        in_specs=(states, states) + (cut,) * 9,
        out_specs=(P("rep", "dp", None),) * 9,
        check_vma=False,
    )
```

```python
import jax
import jax.numpy as jnp
from jax import lax
from jax.experimental import pallas as pl
from jax.experimental.pallas import tpu as pltpu
from jax.sharding import PartitionSpec as P

F32, BF16 = jnp.float32, jnp.bfloat16
MESH = pl.DeviceIdType.MESH
TOKENS, D, HALF, PART = 1024, 512, 4096, 1024
PAIR, STEP = 2 * TOKENS, 256
MIB = 2**20


def nt(a, b):
    return lax.dot_general(a, b, (((1,), (1,)), ((), ())), preferred_element_type=F32)


def nn(a, b):
    return jnp.dot(a, b, preferred_element_type=F32)


def scaled(wide):
    return lax.rsqrt(jnp.mean(wide * wide, -1, keepdims=True) + 1e-6)


def turned(a):
    return a.astype(F32).T.astype(BF16)


def blocks(body, low=0, high=PAIR // STEP):
    def one(b, _):
        body(pl.ds(pl.multiple_of(b * STEP, STEP), STEP), pl.ds(pl.multiple_of((b * STEP + TOKENS) % PAIR, STEP), STEP))
        return 0

    lax.fori_loop(low, high, one, 0)


def places():
    me, r = lax.axis_index("dp"), lax.axis_index("rep")
    c, z, y = me % 2, me // 2 % 4, me // 8
    row = [(r, y * 8 + (z + k) % 4 * 2 + c) for k in range(4)]
    return me, r, c, z, y, row, (r, (1 - y) * 8 + z * 2 + c), (r, me // 2 * 2 + 1 - c)


def greet(peers):
    barrier = pltpu.get_barrier_semaphore()
    for peer in peers:
        pl.semaphore_signal(barrier, inc=1, device_id=peer, device_id_type=MESH)
    pl.semaphore_wait(barrier, len(peers))


def remote(src, dst, send_sem, recv_sem, to):
    return pltpu.make_async_remote_copy(src_ref=src, dst_ref=dst, send_sem=send_sem, recv_sem=recv_sem, device_id=to, device_id_type=MESH)


def gather_kernel(
    w_gate, w_up, sd, x, dy, wgu, wd, out_h1, out_a0, out_a1, out_at0, out_at1, out_dy, out_dyt,
    give, sgu, vg, vu, vd, acc, got, h, a, at, h1, a1, at1, dys, dyt, send_sem, recv_sem, own_sem, load_sem, pair_sem, out_sem,
):
    me, r, c, z, y, row, across, partner = places()
    chip, other = me // 2, (1 - r, me)

    def split(j, _):
        to, own, its = (pl.ds(pl.multiple_of(at * D, D), D) for at in (j, 2 * j + c, 2 * j + 1 - c))
        for n in range(2):
            for m, w in enumerate((w_gate, w_up)):
                give[n, m, :, to] = w[n, :, its]
                sgu[n, m, c, :, to] = w[n, :, own]
        return 0

    lax.fori_loop(0, 8, split, 0)
    greet(row[1:] + [across, other, partner])

    mine, theirs = pl.ds(0, TOKENS), pl.ds(TOKENS, TOKENS)
    swaps = [(give, sgu.at[:, :, c]), (x, h.at[theirs]), (dy, dys.at[theirs])]
    swaps = [remote(src, dst, pair_sem.at[0, i], pair_sem.at[1, i], partner) for i, (src, dst) in enumerate(swaps)]
    stays = [(x, h.at[mine]), (dy, dys.at[mine])]
    stays = [pltpu.make_async_copy(src, dst, load_sem.at[i]) for i, (src, dst) in enumerate(stays)]
    for one in swaps + stays:
        one.start()

    def gate(ref, i):
        return ref.at[0] if i == 2 else ref.at[1, pl.ds(i * 16 - 48, 16)]

    def place(n, i, chip, half):
        if i > 1:
            return gate(wgu.at[n, 0, chip], i)
        return wd.at[n, chip, half] if i else wgu.at[n, 1, chip, half]

    def source(n, i):
        if i > 1:
            return gate(sgu.at[n, 0], i)
        return sd.at[n, r] if i else sgu.at[n, 1, r]

    def origin(slot):
        return (y if slot < 3 else 1 - y) * 4 + (z + (3 if slot < 3 else 7) - slot) % 4

    started = []

    def start(j, src, dst, slot, to):
        one = remote(src, dst, send_sem.at[j * 14 + slot], recv_sem.at[j * 14 + slot], to)
        one.start()
        started.append(one)

    def arrived(j, slot):
        n, i = divmod(j, 5)
        block = place(n, i, origin(slot % 7), 1 - r if slot > 6 else r)
        remote(block, block, send_sem.at[j * 14 + slot], recv_sem.at[j * 14 + slot], other).wait_recv()
        return block

    def begin(j):
        n, i = divmod(j, 5)
        for k in (1, 3, 2):
            start(j, source(n, i), place(n, i, chip, r), k - 1, row[k])

    def own_over_y(j):
        n, i = divmod(j, 5)
        start(j, source(n, i), place(n, i, chip, r), 3, across)

    def ahead(j):
        begin(j)
        own_over_y(j)

    def relay(j, slot):
        block = arrived(j, slot)
        if slot < 3:
            start(j, block, block, 4 + slot, across)
        if j % 5 < 2:
            start(j, block, block, 7 + slot, other)

    ahead(1)
    swaps[0].wait()
    owns = []
    for n in range(2):
        for i, (ref, to) in enumerate(((sgu.at[n, 0], wgu.at[n, 0]), (sgu.at[n, 1], wgu.at[n, 1]), (sd.at[n], wd.at[n]))):
            owns.append(pltpu.make_async_copy(ref, to.at[chip], own_sem.at[3 * n + i]))
            owns[-1].start()
    ahead(0)
    for j in (2, 3, 4):
        own_over_y(j)

    saved = []

    def save(src, dst):
        saved.append(pltpu.make_async_copy(src, dst, out_sem.at[len(saved)]))
        saved[-1].start()

    def first_norm():
        for one in swaps[1:] + stays:
            one.wait()

        def body(rows, _):
            wide = h[rows, :].astype(F32)
            normed = (wide * scaled(wide)).astype(BF16)
            a[rows, :] = normed
            at[:, rows] = turned(normed)
            dyt[:, rows] = turned(dys[rows, :])

        blocks(body)
        save(a, out_a0)
        save(at, out_at0)
        save(dys, out_dy)
        save(dyt, out_dyt)

    def from_row(j):
        for slot in (0, 2, 1):
            relay(j, slot)

    def from_across(j):
        for slot in (3, 4, 6, 5):
            relay(j, slot)

    from_row(1)
    begin(2)
    first_norm()
    from_row(0)
    begin(3)
    begin(4)
    from_across(1)
    from_row(2)
    ahead(6)
    from_across(0)
    from_row(3)
    from_row(4)
    ahead(5)
    from_across(2)
    from_across(3)
    from_across(4)
    for one in owns:
        one.wait()
    for j in (1, 0):
        for slot in range(7, 14):
            arrived(j, slot)
    loads = [(wgu.at[0, 0], vg), (wgu.at[0, 1], vu), (wd.at[0], vd)]
    loads = [pltpu.make_async_copy(src, dst, load_sem.at[i]) for i, (src, dst) in enumerate(loads)]
    for one in loads:
        one.start()
    from_row(6)
    ahead(7)
    for one in loads:
        one.wait()

    def forward(t):
        cols = slice(t * D, t * D + D)

        def body(b, _):
            rows = pl.ds(pl.multiple_of(b * D, D), D)
            gate = nn(a[rows, :], vg[:, :, :, cols].reshape(D, D))
            up = nn(a[rows, :], vu[:, :, :, cols].reshape(D, D))
            part = nn((gate * jax.nn.sigmoid(gate) * up).astype(BF16), vd[t].reshape(D, D))
            acc[rows, :] = acc[rows, :] + part if t else part
            return 0

        lax.fori_loop(0, PAIR // D, body, 0)

    later = {1: (from_row, 5), 2: (ahead, 8), 3: (from_across, 6), 5: (from_across, 5), 6: (from_row, 7)}
    for t in range(8):
        forward(t)
        if t in later:
            later[t][0](later[t][1])
    ahead(9)
    swap = remote(acc, got, pair_sem.at[0, 3], pair_sem.at[1, 3], partner)
    swap.start()
    from_across(7)
    swap.wait()

    def second_norm(rows, theirs):
        state = h[rows, :] + (acc[rows, :] + got[theirs, :]).astype(BF16)
        wide = state.astype(F32)
        normed = (wide * scaled(wide)).astype(BF16)
        h1[rows, :] = state
        a1[rows, :] = normed
        at1[:, rows] = turned(normed)

    blocks(second_norm)
    save(h1, out_h1)
    save(a1, out_a1)
    save(at1, out_at1)
    from_row(8)
    from_row(9)
    from_across(8)
    from_across(9)
    for j in (6, 5):
        for slot in range(7, 14):
            arrived(j, slot)
    for one in saved:
        one.wait()
    for one in started:
        one.wait_send()


def shape(*dims, dtype=BF16):
    return jax.ShapeDtypeStruct(dims, dtype)


ANY, VMEM = pl.BlockSpec(memory_space=pl.ANY), pl.BlockSpec(memory_space=pltpu.VMEM)


def bf(*dims):
    return pltpu.VMEM(dims, BF16)


def wide(*dims):
    return pltpu.VMEM(dims, F32)


def dma(*dims):
    return pltpu.SemaphoreType.DMA(dims)


def gather(*args):
    rows, cols = (PAIR, D), (D, PAIR)
    return pl.pallas_call(
        gather_kernel,
        out_shape=(shape(2, 2, 8, 2, 32, HALF), shape(2, 8, 2, 256, D)) + tuple(shape(*s) for s in (rows, rows, rows, cols, cols, rows, cols)),
        in_specs=[VMEM] * 5,
        out_specs=(ANY,) * 9,
        scratch_shapes=[
            bf(2, 2, 32, HALF), bf(2, 2, 2, 32, HALF), bf(8, 2, 32, HALF), bf(8, 2, 32, HALF), bf(8, 2, 256, D), wide(*rows), wide(*rows),
            bf(*rows), bf(*rows), bf(*cols), bf(*rows), bf(*rows), bf(*cols), bf(*rows), bf(*cols),
            dma(140), dma(140), dma(6), dma(3), dma(2, 4), dma(7),
        ],
        compiler_params=pltpu.CompilerParams(collective_id=0, has_side_effects=True, vmem_limit_bytes=60 * MIB),
        name="gather_forward",
    )(*args)


def backward_kernel(
    wgu, wd, a0, a1, at0, at1, dy, dyt, h1, out_d, out_g, square, from_y_d, from_y_g, from_z_d, from_z_g,
    a, at, by_h, by_ht, by_a, got, act, by_gate, by_up, vgu, vd, unit_d, unit_g, stage_yd, stage_yg, sent_d, sent_g, own_d, own_g,
    stage_zd, stage_zg, whole, sums, y_send, y_recv, z_send, z_recv, stage_sem, load_sem, w_sem, pair_sem, core_sem, sum_sem,
):
    me, r, c, z, y, row, across, partner = places()

    def trio(d, g):
        return [d, g.at[0], g.at[1]]

    unit, from_y, from_z, stage_y = trio(unit_d, unit_g), trio(from_y_d, from_y_g), trio(from_z_d, from_z_g), trio(stage_yd, stage_yg)
    stage_z, sent, own = trio(stage_zd, stage_zg), trio(sent_d, sent_g), trio(own_d, own_g)

    def over_y(k, i):
        src = unit[i].at[k % 2, pl.ds((1 - y) * 4, 4)]
        return remote(src, from_y[i].at[k], y_send.at[k * 3 + i], y_recv.at[k * 3 + i], across)

    def over_z(k, i, hop):
        at = (k * 3 + i) * 3 + hop - 1
        return remote(sent[i].at[k % 2, hop - 1], from_z[i].at[k, hop - 1], z_send.at[at], z_recv.at[at], row[hop])

    def over_cores(k, i):
        at = (i - 1) * 8 + k
        return remote(whole.at[i - 1, k, 1 - c], out_g.at[i - 1, k, c], core_sem.at[0, at], core_sem.at[1, at], partner)

    def stage_of_y(k, i):
        return pltpu.make_async_copy(from_y[i].at[k], stage_y[i], stage_sem.at[i])

    def stage_of_z(k, i):
        return pltpu.make_async_copy(from_z[i].at[k], stage_z[i], stage_sem.at[3 + i])

    def fetch_y(k, i):
        over_y(k, i).wait_recv()
        stage_of_y(k, i).start()

    def add_y(k, i):
        stage_of_y(k, i).wait()
        over_y(k, i).wait_send()
        for hop in (2, 1, 3, 0):
            to = (z + hop) % 4
            total = unit[i][k % 2, y * 4 + to].astype(F32) + stage_y[i][to].astype(F32)
            if hop:
                sent[i][k % 2, hop - 1] = total.astype(BF16)
                over_z(k, i, hop).start()
            else:
                own[i][k % 2] = total

    def fetch_z(k, i):
        for hop in (1, 3, 2):
            over_z(k, i, hop).wait()
        stage_of_z(k, i).start()

    def add_z(k, i):
        stage_of_z(k, i).wait()
        total = own[i][k % 2]
        for hop in range(3):
            total = total + stage_z[i][hop].astype(F32)
        total = total.astype(BF16)
        if i:
            whole[i - 1, k] = total
            out_g[i - 1, k, c] = whole[i - 1, k, c]
            over_cores(k, i).start()
        else:
            out_d[k] = total
        g = total.astype(F32)
        g = jnp.sum((g * g).reshape(-1, 8, g.shape[-1]), 0)
        parts = [g[:, j : j + 128] for j in range(0, g.shape[-1], 128)]
        sums[0] += sum(parts[1:], parts[0])

    lags = ((add_y, 4), (fetch_y, 3), (add_z, 8), (fetch_z, 7))

    def advance(k, i, known):
        for step, lag in lags:
            back, which = divmod(i - lag, 3)

            @pl.when(known | (k + back >= 0))
            def _():
                step(k + back, which)

    def weights(n, q):
        slot, some = q % 2, pl.ds(pl.multiple_of(q * 128, 128), 128)
        copies = [pltpu.make_async_copy(wd.at[n, :, q // 2, pl.ds(pl.multiple_of(q % 2 * 128, 128), 128)], vd.at[slot], w_sem.at[slot, 8])]
        for j in range(8):
            src = wgu.at[n, :, :, :, :, pl.ds(pl.multiple_of(j * D + q * 128, 128), 128)]
            copies.append(pltpu.make_async_copy(src, vgu.at[slot, :, :, :, :, pl.ds(j * 128, 128)], w_sem.at[slot, j]))
        return copies

    def begin(copies):
        for one in copies:
            one.start()

    def finish(copies):
        for one in copies:
            one.wait()

    def fill(pairs):
        copies = [pltpu.make_async_copy(src, dst, load_sem.at[i]) for i, (src, dst) in enumerate(pairs)]
        begin(copies)
        return copies

    sums[0] = jnp.zeros_like(sums[0])
    loads = fill([(a1, a), (dy, by_h), (at1, at), (dyt, by_ht)])
    begin(weights(1, me * 0))
    greet(row[1:] + [across, partner])
    finish(loads)

    def layer(n):
        def part(q, _):
            k, slot = (1 - n) * 4 + q, q % 2
            finish(weights(n, q))
            pl.when(q < 3)(lambda: begin(weights(n, q + 1)))
            if n:
                pl.when(q == 3)(lambda: begin(weights(0, q - 3)))

            def body(rows, _):
                gate_w, up_w = (vgu[slot, j].reshape(D, PART) for j in range(2))
                gate, up = nn(a[rows, :], gate_w), nn(a[rows, :], up_w)
                by_act = nt(by_h[rows, :], vd[slot].reshape(PART, D)).astype(BF16).astype(F32)
                sig = jax.nn.sigmoid(gate)
                silu = gate * sig
                act[rows, :] = (silu * up).astype(BF16)
                g = (by_act * up * (sig + silu * (1.0 - sig))).astype(BF16)
                u = (by_act * silu).astype(BF16)
                by_gate[rows, :] = g
                by_up[rows, :] = u
                if n:
                    total = nt(g, gate_w) + nt(u, up_w)

                    @pl.when(q == 0)
                    def _():
                        by_a[rows, :] = total

                    @pl.when(q > 0)
                    def _():
                        by_a[rows, :] += total

            blocks(body, 0, 4)
            advance(k, 0, False)
            blocks(body, 4)
            for i, (left, right) in enumerate(((by_ht, act), (at, by_gate), (at, by_up))):

                def columns(j, _):
                    cols = pl.ds(pl.multiple_of(j * STEP, STEP), STEP)
                    g = nn(left[...], right[:, cols]).astype(BF16)
                    if i:
                        unit_g[i - 1, k % 2, :, :, :, cols] = g.reshape(8, 2, 32, STEP)
                    else:
                        unit_d[k % 2, 2 * j] = g[:, :128]
                        unit_d[k % 2, 2 * j + 1] = g[:, 128:]
                    return 0

                lax.fori_loop(0, PART // STEP, columns, 0)
                over_y(k, i).start()
                if i != 1:
                    advance(k, 1 + i // 2, False)
            return 0

        lax.fori_loop(0, 4, part, 0)

    layer(1)
    swap = remote(by_a, got, pair_sem.at[0], pair_sem.at[1], partner)
    swap.start()
    loads = fill([(a0, a), (at0, at)])
    swap.wait()

    def between(rows, theirs):
        g = (by_a[rows, :] + got[theirs, :]).astype(BF16).astype(F32)
        state = h1[rows, :].astype(F32)
        scale = scaled(state)
        inner = jnp.mean(g * state, -1, keepdims=True)
        total = by_h[rows, :] + (g * scale - state * (scale * scale * scale * inner)).astype(BF16)
        by_h[rows, :] = total
        by_ht[:, rows] = turned(total)

    blocks(between)
    finish(loads)
    layer(0)
    for s in range(24, 32):
        for step, lag in lags:
            if s - lag < 24:
                step(*divmod(s - lag, 3))

    def share(src, at, to):
        one = remote(sums.at[src], sums.at[at], sum_sem.at[0, at], sum_sem.at[1, at], to)
        one.start()
        return one

    share(0, 3, partner).wait()
    sums[1] = sums[0] + sums[3]
    share(1, 4, across).wait()
    sums[2] = sums[1] + sums[4]
    finish([share(2, 4 + hop, row[hop]) for hop in (1, 2, 3)])
    square[...] = sums[2] + sums[5] + sums[6] + sums[7]
    for i in (1, 2):
        for k in range(8):
            over_cores(k, i).wait()


def backward(wgu, wd, a0, a1, at0, at1, dy, dyt, h1):
    rows, cols, g, d = (PAIR, D), (D, PAIR), (2, 32, PART), (D, 128)
    part = (PAIR, PART)
    return pl.pallas_call(
        backward_kernel,
        out_shape=(
            shape(8, *d), shape(2, 8, *g), shape(8, 128, dtype=F32), shape(8, 4, *d), shape(2, 8, 4, *g), shape(8, 3, *d), shape(2, 8, 3, *g),
        ),
        in_specs=[ANY] * 8 + [VMEM],
        out_specs=(VMEM,) * 3 + (ANY,) * 4,
        scratch_shapes=[
            bf(*rows), bf(*cols), bf(*rows), bf(*cols), wide(*rows), wide(*rows), bf(*part), bf(*part), bf(*part),
            bf(2, 2, 8, 2, 32, PART), bf(2, 8, 128, D), bf(2, 8, *d), bf(2, 2, 8, *g), bf(4, *d), bf(2, 4, *g), bf(2, 3, *d), bf(2, 2, 3, *g),
            wide(2, *d), wide(2, 2, *g), bf(3, *d), bf(2, 3, *g), bf(2, 8, *g), wide(8, 8, 128),
            dma(24), dma(24), dma(72), dma(72), dma(6), dma(4), dma(2, 9), dma(2), dma(2, 16), dma(2, 8),
        ],
        compiler_params=pltpu.CompilerParams(collective_id=1, has_side_effects=True, vmem_limit_bytes=63 * MIB),
        name="backward_sum",
    )(wgu, wd, a0, a1, at0, at1, dy, dyt, h1)


def adamw(w, m, v, g):
    m = 0.9 * m + 0.1 * g
    v = 0.95 * v + 0.05 * g * g
    step = m * lax.rsqrt(v + 1e-8) + 0.1 * w
    return (w - 0.02 * step).astype(BF16), m, v


def update_kernel(count, square, by_d, by_gate, by_up, *refs):
    olds, news = refs[:9], refs[9:]
    factor = jnp.minimum(1.0, 0.5 * lax.rsqrt(jnp.sum(square[...]) / count + 1e-30))

    def columns(g):
        pieces = [(j, core, q) for j in range(2) for core in range(2) for q in range(4)]
        return jnp.concatenate([g[0, q, core, :, j * 128 : j * 128 + 128] for j, core, q in pieces], 1)

    for i, g in enumerate((columns(by_gate), columns(by_up), by_d[0].astype(F32).T)):
        w, m, v = (ref[0] for ref in olds[i::3])
        for ref, one in zip(news[i::3], adamw(w.astype(F32), m, v, g.astype(F32) * factor), strict=True):
            ref[0] = one


def update(square, by_d, by_g, arrays):
    grid, layers = (arrays[0].shape[0], 4), arrays[0].shape[0]
    up = pl.BlockSpec((1, 32, 8192 // 4), lambda n, s: (n, 0, s))
    down = pl.BlockSpec((1, 128, D), lambda n, s: (n, s, 0))
    own = [up, up, down] * 3
    g = [pl.BlockSpec((1, 4, 2, 32, STEP), lambda n, s, i=i: (i, 1 - n, 0, 0, s)) for i in range(2)]
    return pl.pallas_call(
        lambda *refs: update_kernel(16 * sum(w.size for w in arrays[:3]), *refs),
        grid=grid,
        out_shape=tuple(jax.ShapeDtypeStruct(w.shape, w.dtype) for w in arrays),
        in_specs=[pl.BlockSpec((8, 128), lambda n, s: (0, 0)), pl.BlockSpec((1, D, 128), lambda n, s: ((1 - n) * 4 + s, 0, 0)), *g, *own],
        out_specs=tuple(own),
        name="update",
    )(square, by_d, by_g, by_g, *arrays)


def solution(mesh):
    def step(x, dy, *arrays):
        w_gate, w_up, w_down = arrays[:3]
        layers = w_gate.shape[0]
        wgu, wd, h1, *rest = gather(w_gate, w_up, w_down.reshape(layers, 2, 256, D), x[0], dy[0])
        by_d, by_g, square = backward(wgu, wd, *rest, h1)[:3]
        return tuple(update(square, by_d, by_g, arrays))

    states, cut = P(("rep", "dp"), None, None), P(None, "dp", None)
    return jax.shard_map(
        step,
        mesh=mesh,
        in_specs=(states, states) + (cut,) * 9,
        out_specs=(P("rep", "dp", None),) * 9,
        check_vma=False,
    )
```
